32 devices in a mesh: dp: 8 (over z, x), rep: 4 (over y, core).
Axes of the slice: x: 2, y: 2, z: 4, core: 2. Of those that a mesh axis runs over, the one named last changes fastest.
Arguments:
- token_inputs: bfloat16 [16384, 2048], P(('dp', 'rep')), may hold values from -12 to 12
- cotangent: bfloat16 [16384, 2048], P(('dp', 'rep')), may hold values from -6 to 6
- gate_preact: bfloat16 [16384, 768], P(('dp', 'rep')), may hold values from -6 to 6
- up_preact: bfloat16 [16384, 768], P(('dp', 'rep')), may hold values from -6 to 6
- down_weight: bfloat16 [2, 768, 2048], P(None, None, 'dp'), may hold values from -0.21875 to 0.21875
- block_expert: int32 [128], P(('dp', 'rep')), may hold values from 0 to 1
- block_count: int32 [128], P(('dp', 'rep')), may hold values from 1 to 128, as said below
Outputs:
- update: bfloat16 [2, 3, 768, 2048], P(None, None, None, 'dp')
The draws below stay inside these ranges and needn't reach their ends.
Inputs may be any that keep to these rules, and one draw needn't show every extreme that they name: `block_count`: live rows of a block, at most 128; in every draw some block is full.
All inputs are finite; a program needn't handle non-finite values.
Results may differ from the reference program's by a relative error of at most 0.02.
Values may be sent and summed in bfloat16 or wider, within the bound.
A program may use at most 128 MiB of HBM per device.

```python
import jax
import jax.numpy as jnp
from jax import lax

D = 2048
F = 768
EXPERTS = 2
BLOCK = 128
BLK = 4
ITERS = 2
ROWS = 16384
BLOCKS_ALL = 128
N_DP = 8
N_REP = 4


def draw_block_count(key, part):
    counts = jax.random.randint(key, (BLOCKS_ALL,), max(1, BLOCK // 4), BLOCK + 1, dtype=jnp.int32)
    chosen = jax.random.randint(jax.random.fold_in(key, 7), (), 0, BLOCKS_ALL, dtype=jnp.int32)
    return jnp.where(jnp.arange(BLOCKS_ALL, dtype=jnp.int32) == chosen, jnp.int32(BLOCK), counts)


def draw_token_inputs(key, part):
    column = jnp.arange(D, dtype=jnp.float32) / jnp.float32(max(D - 1, 1))
    ratio = 2.5
    base = jnp.clip(jax.random.normal(key, (ROWS, D), jnp.float32), -6.0, 6.0)
    scale = jnp.exp(jnp.log(jnp.float32(ratio)) * (column - 0.5))
    return (base * scale[None, :]).astype(jnp.bfloat16)


def plant(values, own_key, smallest, top_value):
    spot = [jax.random.randint(jax.random.fold_in(own_key, axis), (), 0, length) for axis, length in enumerate(values.shape)]
    longest = values.shape.index(max(values.shape))
    neighbour = spot[:longest] + [(spot[longest] + 1) % values.shape[longest]] + spot[longest + 1:]
    return values.at[tuple(spot)].set(smallest).at[tuple(neighbour)].set(top_value)


def spiked(values, own_key, source, target, shards_of, factor):
    def block_of(dim):
        return (jnp.arange(values.shape[dim]) // (values.shape[dim] // shards_of)).reshape((-1,) + (1,) * (values.ndim - 1 - dim))

    first = jax.random.permutation(own_key, shards_of)[block_of(target)]
    far = (block_of(target) + shards_of // 2) % shards_of
    return jnp.where((block_of(source) == first) | (block_of(source) == far), factor * values, values)


def level_of(stream_key, extent, shards, low, high):
    factor_of, own = 1.0, jax.random.fold_in(stream_key, 6)
    for position, blocks in shards:
        draws = jnp.exp(jax.random.uniform(jax.random.fold_in(own, position), (blocks,), jnp.float32, low / len(shards), high / len(shards)))
        factor_of = factor_of * jnp.repeat(draws, extent[position] // blocks).reshape([-1 if axis == position else 1 for axis in range(len(extent))])
    return factor_of


def normal_values(rng, dims, scale, most, pieces=(), kind=jnp.bfloat16):
    values = scale * jax.random.normal(rng, dims, jnp.float32)
    if pieces:
        values = values * level_of(rng, dims, pieces, -0.22, 0.18)
    return jnp.clip(values, -most, most).astype(kind)


def noise_with(key, extent, deviation, bound, pieces, heavy, held_as=jnp.bfloat16):
    drawn = deviation * jax.random.normal(key, extent, jnp.float32)
    if pieces:
        drawn = drawn * level_of(key, extent, pieces, -0.22, 0.18)
    return jnp.clip(spiked(drawn, jax.random.fold_in(key, 3), *heavy), -bound, bound).astype(held_as)


def setup_inputs(seed: int = 0) -> dict:
    key_list = jax.random.split(jax.random.key(seed), 8)
    token_inputs = draw_token_inputs(jax.random.fold_in(key_list[7], 71), 0)
    cotangent = noise_with(key_list[1], (ROWS, D), 1.0, 6.0, ((0, 32),), (0, 1, 32, 2.75))
    gate_preact = normal_values(key_list[2], (ROWS, F), 1.0, 6.0, ((0, 32),))
    up_preact = normal_values(key_list[3], (ROWS, F), 1.0, 6.0, ((0, 32),))
    down_weight = normal_values(key_list[4], (EXPERTS, F, D), F ** -0.5, 0.21875, ((2, 8),))
    block_expert = plant(jax.random.randint(key_list[5], (BLOCKS_ALL,), 0, EXPERTS), jax.random.fold_in(key_list[5], 1), 0, EXPERTS - 1).astype(jnp.int32)
    block_count = draw_block_count(jax.random.fold_in(key_list[7], 71), 0)
    return dict(token_inputs=token_inputs, cotangent=cotangent, gate_preact=gate_preact, up_preact=up_preact, down_weight=down_weight, block_expert=block_expert, block_count=block_count)


ns_first = 3.4445
ns_second = -4.775
ns_third = 2.0315
norm_eps = 1e-07

def device_partial(inputs, cotangent, gate_preact, up_preact, down_weight, experts, counts):
    blocks = counts.shape[0]
    width = inputs.shape[1]
    hidden_width = gate_preact.shape[1]
    inputs = inputs.reshape(blocks, BLOCK, width)
    cotangent = cotangent.reshape(blocks, BLOCK, width)
    gate = gate_preact.reshape(blocks, BLOCK, hidden_width).astype(jnp.float32)
    upper = up_preact.reshape(blocks, BLOCK, hidden_width).astype(jnp.float32)
    live_rows = jnp.arange(BLOCK, dtype=jnp.int32)[None, :] < counts[:, None]
    masked = jnp.where(live_rows[:, :, None], cotangent, jnp.zeros_like(cotangent))
    sigmoid_gate = jax.nn.sigmoid(gate)
    hidden = (gate * sigmoid_gate * upper).astype(jnp.bfloat16)
    chosen = jnp.take(down_weight, experts, axis=0)
    back = jnp.einsum('brd,bfd->brf', masked.astype(jnp.float32), chosen.astype(jnp.float32))
    grad_gate = (back * upper * sigmoid_gate * (1.0 + gate * (1.0 - sigmoid_gate))).astype(jnp.bfloat16)
    grad_up = (back * gate * sigmoid_gate).astype(jnp.bfloat16)
    left = jnp.stack([grad_gate, grad_up, hidden], 1).astype(jnp.float32)
    right = jnp.stack([inputs, inputs, masked], 1).astype(jnp.float32)
    per_block = jnp.einsum('bmrf,bmrd->bmfd', left, right)
    onehot = (experts[:, None] == jnp.arange(EXPERTS, dtype=jnp.int32)[None, :]).astype(jnp.float32)
    partial_value = jnp.einsum('be,bmfd->emfd', onehot, per_block, precision=lax.Precision.HIGHEST)
    return partial_value.astype(jnp.bfloat16)

def reference(token_inputs, cotangent, gate_preact, up_preact, down_weight, block_expert, block_count):
    devices_all = N_DP * N_REP
    rows_dev = BLK * BLOCK

    def add_device(total, index):
        first = (index * rows_dev).astype(jnp.int32)
        first_block = (index * BLK).astype(jnp.int32)
        partial_value = device_partial(lax.dynamic_slice_in_dim(token_inputs, first, rows_dev, 0), lax.dynamic_slice_in_dim(cotangent, first, rows_dev, 0), lax.dynamic_slice_in_dim(gate_preact, first, rows_dev, 0), lax.dynamic_slice_in_dim(up_preact, first, rows_dev, 0), down_weight, lax.dynamic_slice_in_dim(block_expert, first_block, BLK, 0), lax.dynamic_slice_in_dim(block_count, first_block, BLK, 0))
        return (total + partial_value.astype(jnp.float32), None)
    start_total = jnp.zeros((EXPERTS, 3, F, D), jnp.float32)
    grad, unused = lax.scan(add_device, start_total, jnp.arange(devices_all, dtype=jnp.int32))
    squares = lax.optimization_barrier(jnp.sum(grad * grad, axis=(2, 3)))
    current = (grad / (jnp.sqrt(squares) + norm_eps)[:, :, None, None]).astype(jnp.bfloat16)
    column_width = D // N_DP
    result = None
    for sweep in range(ITERS):
        as_float = current.astype(jnp.float32)
        split = as_float.reshape(EXPERTS, 3, F, N_DP, column_width)

        def add_columns(total, index):
            block_cols = lax.dynamic_index_in_dim(split, index, 3, False)
            term = jnp.einsum('emfd,emgd->emfg', block_cols, block_cols).astype(jnp.bfloat16)
            return (total + lax.optimization_barrier(term).astype(jnp.float32), None)
        gram, unused = lax.scan(add_columns, jnp.zeros((EXPERTS, 3, F, F), jnp.float32), jnp.arange(N_DP, dtype=jnp.int32))
        gram_half = gram.astype(jnp.bfloat16).astype(jnp.float32)
        squared = jnp.einsum('emfg,emgh->emfh', gram_half, gram_half)
        poly = (ns_second * gram + ns_third * squared).astype(jnp.bfloat16)
        newer = ns_first * as_float + jnp.einsum('emfg,emgd->emfd', poly.astype(jnp.float32), as_float)
        if sweep + 1 < ITERS:
            current = newer.astype(jnp.bfloat16)
        else:
            result = (jnp.sqrt(jnp.float32(D)) * newer).astype(jnp.bfloat16)
    return result
```

```python
import functools

import jax
import jax.numpy as jnp
from jax import lax
from jax.experimental import pallas as pl
from jax.experimental.pallas import tpu as pltpu
from jax.sharding import PartitionSpec as P

D = 2048
ITERS = 2
MESH = pl.DeviceIdType.MESH

ns_first = 3.4445
ns_second = -4.775
ns_third = 2.0315
norm_eps = 1e-07


def rep_sum_kernel(
    n_chunks, parts, out, local, near, summed, far,
    load_sem, near_send, near_recv, far_send, far_recv, store_sem,
):
    dp = lax.axis_index("dp")
    rep = lax.axis_index("rep")
    pair = rep + 1 - 2 * lax.rem(rep, 2)
    other = lax.rem(rep + 2, 4)
    other_pair = lax.rem(pair + 2, 4)

    def near_copy(slot, chunk):
        part = other_pair if slot == 0 else pair
        return pltpu.make_async_remote_copy(
            src_ref=parts.at[part, chunk],
            dst_ref=near.at[slot, chunk],
            send_sem=near_send.at[slot, chunk],
            recv_sem=near_recv.at[slot, chunk],
            device_id=(dp, pair),
            device_id_type=MESH,
        )

    def load(slot, chunk):
        part = other if slot == 0 else rep
        return pltpu.make_async_copy(
            parts.at[part, chunk], local.at[slot, chunk], load_sem.at[slot, chunk]
        )

    def far_copy(chunk):
        return pltpu.make_async_remote_copy(
            src_ref=summed.at[chunk],
            dst_ref=far.at[chunk],
            send_sem=far_send.at[chunk],
            recv_sem=far_recv.at[chunk],
            device_id=(dp, other),
            device_id_type=MESH,
        )

    def store(chunk):
        return pltpu.make_async_copy(local.at[1, chunk], out.at[chunk], store_sem.at[chunk])

    for slot in range(2):

        @pl.loop(0, n_chunks)
        def _(chunk, slot=slot):
            near_copy(slot, chunk).start()
            load(slot, chunk).start()

    @pl.loop(0, n_chunks)
    def _(chunk):
        load(0, chunk).wait()
        near_copy(0, chunk).wait_recv()
        summed[chunk] = (
            local[0, chunk].astype(jnp.float32) + near[0, chunk].astype(jnp.float32)
        ).astype(jnp.bfloat16)
        far_copy(chunk).start()

    @pl.loop(0, n_chunks)
    def _(chunk):
        load(1, chunk).wait()
        near_copy(1, chunk).wait_recv()
        far_copy(chunk).wait_recv()
        local[1, chunk] = (
            local[1, chunk].astype(jnp.float32)
            + near[1, chunk].astype(jnp.float32)
            + far[chunk].astype(jnp.float32)
        ).astype(jnp.bfloat16)
        store(chunk).start()

    @pl.loop(0, n_chunks)
    def _(chunk):
        near_copy(0, chunk).wait_send()
        near_copy(1, chunk).wait_send()
        far_copy(chunk).wait_send()
        store(chunk).wait()


def rep_sum(value, rows):
    width = value.shape[-1]
    parts = value.reshape(4, -1, rows, width)
    n_chunks = parts.shape[1]
    block = (n_chunks, rows, width)
    summed = pl.pallas_call(
        functools.partial(rep_sum_kernel, n_chunks),
        out_shape=jax.ShapeDtypeStruct(block, jnp.bfloat16),
        in_specs=[pl.BlockSpec(memory_space=pl.ANY)],
        out_specs=pl.BlockSpec(memory_space=pl.ANY),
        scratch_shapes=[
            pltpu.VMEM((2,) + block, jnp.bfloat16),
            pltpu.VMEM((2,) + block, jnp.bfloat16),
            pltpu.VMEM(block, jnp.bfloat16),
            pltpu.VMEM(block, jnp.bfloat16),
            pltpu.SemaphoreType.DMA((2, n_chunks)),
            pltpu.SemaphoreType.DMA((2, n_chunks)),
            pltpu.SemaphoreType.DMA((2, n_chunks)),
            pltpu.SemaphoreType.DMA((n_chunks,)),
            pltpu.SemaphoreType.DMA((n_chunks,)),
            pltpu.SemaphoreType.DMA((n_chunks,)),
        ],
        compiler_params=pltpu.CompilerParams(has_side_effects=True),
        cost_estimate=pl.CostEstimate(
            flops=value.size * 1000, bytes_accessed=value.size * 2, transcendentals=0
        ),
    )(parts)
    return summed.reshape(n_chunks * rows, width)


def column_block(matrix, source, width, rows=None):
    if len(matrix.shape) == 3:
        return matrix.at[source] if rows is None else matrix.at[source, rows]
    start = source * width
    cols = pl.ds(start if isinstance(start, int) else pl.multiple_of(start, width), width)
    return matrix.at[:, cols] if rows is None else matrix.at[rows, cols]


def gather_kernel(n_dp, first, second, whole, full_send, half_send, full_recv, half_recv):
    dp = lax.axis_index("dp")
    rep = lax.axis_index("rep")
    odd = lax.rem(rep, 2)
    hidden, width = first.shape
    half = second.shape[0]
    owner = n_dp // 4

    def full_copy(source):
        return pltpu.make_async_remote_copy(
            src_ref=first,
            dst_ref=column_block(whole, source, width),
            send_sem=full_send,
            recv_sem=full_recv.at[source],
            device_id=(owner + odd, rep),
            device_id_type=MESH,
        )

    def half_copy(place, source):
        rows = pl.ds(pl.multiple_of(place * half, half), half)
        return pltpu.make_async_remote_copy(
            src_ref=second,
            dst_ref=column_block(whole, source, width, rows),
            send_sem=half_send,
            recv_sem=half_recv.at[place, source],
            device_id=(owner + 2, rep - odd),
            device_id_type=MESH,
        )

    own_full = pltpu.make_async_copy(first, column_block(whole, dp, width), full_send)
    own_half = pltpu.make_async_copy(
        second, column_block(whole, dp, width, pl.ds(0, half)), half_send
    )
    is_full = dp == owner + odd
    is_half = jnp.logical_and(dp == owner + 2, odd == 0)

    @pl.when(is_full)
    def _():
        own_full.start()

    @pl.when(jnp.logical_not(is_full))
    def _():
        full_copy(dp).start()

    @pl.when(is_half)
    def _():
        own_half.start()

    @pl.when(jnp.logical_not(is_half))
    def _():
        half_copy(odd, dp).start()

    @pl.when(is_full)
    def _():
        own_full.wait()
        for source in range(n_dp):

            @pl.when(dp != source)
            def _(source=source):
                full_copy(source).wait_recv()

    @pl.when(jnp.logical_not(is_full))
    def _():
        full_copy(dp).wait_send()

    @pl.when(is_half)
    def _():
        own_half.wait()
        for source in range(n_dp):
            half_copy(1, source).wait_recv()

            @pl.when(dp != source)
            def _(source=source):
                half_copy(0, source).wait_recv()

    @pl.when(jnp.logical_not(is_half))
    def _():
        half_copy(odd, dp).wait_send()


def gather_matrix(first, second, n_dp):
    hidden, width = first.shape
    blocked = width % 128 != 0
    shape = (n_dp, hidden, width) if blocked else (hidden, width * n_dp)
    whole = pl.pallas_call(
        functools.partial(gather_kernel, n_dp),
        out_shape=jax.ShapeDtypeStruct(shape, jnp.bfloat16),
        in_specs=[pl.BlockSpec(memory_space=pltpu.VMEM)] * 2,
        out_specs=pl.BlockSpec(memory_space=pltpu.VMEM),
        scratch_shapes=[
            pltpu.SemaphoreType.DMA,
            pltpu.SemaphoreType.DMA,
            pltpu.SemaphoreType.DMA((n_dp,)),
            pltpu.SemaphoreType.DMA((2, n_dp)),
        ],
        compiler_params=pltpu.CompilerParams(has_side_effects=True),
    )(first, second)
    return whole.transpose(1, 0, 2).reshape(hidden, width * n_dp) if blocked else whole


def spread_kernel(n_dp, matrix, out, held, owner_send, pair_send, far_send, recv, store_sem):
    dp = lax.axis_index("dp")
    rep = lax.axis_index("rep")
    hidden, width = held.shape[1:]
    owner = n_dp // 4
    pair = rep + 1 - 2 * lax.rem(rep, 2)
    other = lax.rem(rep + 2, 4)
    kinds = 3
    matrices = [(expert, kind) for expert in range(2) for kind in range(kinds)]

    def remote(source, index, send_sem, device):
        return pltpu.make_async_remote_copy(
            src_ref=source,
            dst_ref=held.at[index],
            send_sem=send_sem,
            recv_sem=recv.at[index],
            device_id=device,
            device_id_type=MESH,
        )

    def store(index):
        return pltpu.make_async_copy(held.at[index], out.at[index], store_sem.at[index])

    def root_of(expert, kind):
        return 2 * expert + kind % 2

    for index, (expert, kind) in enumerate(matrices):

        @pl.when(jnp.logical_and(dp == owner + kind, rep == root_of(expert, kind)))
        def _(index=index, kind=kind):
            for target in range(n_dp):
                block = column_block(matrix, target, width)

                @pl.when(dp != target)
                def _(target=target, block=block):
                    remote(block, index, owner_send.at[target], (target, rep)).start()

                @pl.when(dp == target)
                def _(target=target, block=block):
                    pltpu.make_async_copy(
                        block, held.at[index], owner_send.at[target]
                    ).start()

    def arrived(index, expert, kind):
        here = dp == owner + kind

        @pl.when(here)
        def _():
            pltpu.make_async_copy(
                column_block(matrix, dp, width),
                held.at[index],
                owner_send.at[dp],
            ).wait()

        @pl.when(jnp.logical_not(here))
        def _():
            remote(held.at[index], index, pair_send.at[index], (dp, pair)).wait_recv()

    for index, (expert, kind) in enumerate(matrices):

        @pl.when(rep == root_of(expert, kind))
        def _(index=index, expert=expert, kind=kind):
            arrived(index, expert, kind)
            remote(held.at[index], index, far_send.at[index], (dp, other)).start()
            remote(held.at[index], index, pair_send.at[index], (dp, pair)).start()
            store(index).start()

    for index, (expert, kind) in enumerate(matrices):

        @pl.when(other == root_of(expert, kind))
        def _(index=index):
            remote(held.at[index], index, pair_send.at[index], (dp, pair)).wait_recv()
            remote(held.at[index], index, pair_send.at[index], (dp, pair)).start()
            store(index).start()

    for index, (expert, kind) in enumerate(matrices):
        root = root_of(expert, kind)

        @pl.when(jnp.logical_and(rep != root, other != root))
        def _(index=index):
            remote(held.at[index], index, pair_send.at[index], (dp, pair)).wait_recv()
            store(index).start()

    for index, (expert, kind) in enumerate(matrices):
        root = root_of(expert, kind)

        @pl.when(jnp.logical_and(dp == owner + kind, rep == root))
        def _(index=index):
            for target in range(n_dp):

                @pl.when(dp != target)
                def _(target=target):
                    remote(
                        column_block(matrix, target, width),
                        index,
                        owner_send.at[target],
                        (target, rep),
                    ).wait_send()

        @pl.when(rep == root)
        def _(index=index):
            remote(held.at[index], index, far_send.at[index], (dp, other)).wait_send()

        @pl.when(jnp.logical_or(rep == root, other == root))
        def _(index=index):
            remote(held.at[index], index, pair_send.at[index], (dp, pair)).wait_send()

        store(index).wait()


def spread_matrix(matrix, n_dp):
    hidden, width = matrix.shape[0], matrix.shape[1] // n_dp
    if width % 128 != 0:
        matrix = matrix.reshape(hidden, n_dp, width).transpose(1, 0, 2)
    return pl.pallas_call(
        functools.partial(spread_kernel, n_dp),
        out_shape=jax.ShapeDtypeStruct((6, hidden, width), jnp.bfloat16),
        in_specs=[pl.BlockSpec(memory_space=pltpu.VMEM)],
        out_specs=pl.BlockSpec(memory_space=pl.ANY),
        scratch_shapes=[
            pltpu.VMEM((6, hidden, width), jnp.bfloat16),
            pltpu.SemaphoreType.DMA((n_dp,)),
            pltpu.SemaphoreType.DMA((6,)),
            pltpu.SemaphoreType.DMA((6,)),
            pltpu.SemaphoreType.DMA((6,)),
            pltpu.SemaphoreType.DMA((6,)),
        ],
        compiler_params=pltpu.CompilerParams(has_side_effects=True),
    )(matrix)


def whole_sweeps(grad, sweeps, scale):
    as_float = grad.astype(jnp.float32)
    norm = jnp.sqrt(jnp.sum(as_float * as_float)) + norm_eps
    current = (as_float / norm).astype(jnp.bfloat16)
    result = None
    for sweep in range(sweeps):
        gram = jnp.einsum("fd,gd->fg", current, current, preferred_element_type=jnp.float32)
        gram_half = gram.astype(jnp.bfloat16)
        squared = jnp.dot(gram_half, gram_half, preferred_element_type=jnp.float32)
        poly = (ns_second * gram + ns_third * squared).astype(jnp.bfloat16)
        newer = ns_first * current.astype(jnp.float32) + jnp.dot(
            poly, current, preferred_element_type=jnp.float32
        )
        if sweep + 1 < sweeps:
            current = newer.astype(jnp.bfloat16)
        else:
            result = (scale * newer).astype(jnp.bfloat16)
    return result


def per_device(
    token_inputs, cotangent, gate_preact, up_preact, down_weight, block_expert, block_count
):
    n_dp = lax.axis_size("dp")
    rep = lax.axis_index("rep")
    odd = lax.rem(rep, 2)
    blocks = block_count.shape[0]
    rows_here = token_inputs.shape[0]
    hidden_width = gate_preact.shape[1]
    half = hidden_width // 2
    width = token_inputs.shape[1]
    block_rows = rows_here // blocks
    experts_here = down_weight.shape[0]

    own_half = lax.dynamic_slice_in_dim(down_weight, odd * half, half, 1)
    weights_own = lax.all_gather(own_half, "dp", axis=2, tiled=True)

    row_place = jnp.arange(rows_here, dtype=jnp.int32) % block_rows
    row_count = jnp.repeat(block_count, block_rows, total_repeat_length=rows_here)
    row_expert = jnp.repeat(block_expert, block_rows, total_repeat_length=rows_here)
    live_rows = row_place < row_count
    masked = jnp.where(live_rows[:, None], cotangent, jnp.zeros_like(cotangent))
    gate = gate_preact.astype(jnp.float32)
    upper = up_preact.astype(jnp.float32)
    sigmoid_gate = jax.nn.sigmoid(gate)
    hidden = (gate * sigmoid_gate * upper).astype(jnp.bfloat16)
    selector = (row_expert[None, :] == jnp.arange(experts_here, dtype=jnp.int32)[:, None]).astype(
        jnp.bfloat16
    )
    hidden_each = hidden[None, :, :] * selector[:, :, None]
    output_part = jnp.einsum(
        "erf,rd->efd", hidden_each, masked, preferred_element_type=jnp.float32
    ).astype(jnp.bfloat16)
    output_sum = rep_sum(output_part, 128)
    weights_own, output_sum = lax.optimization_barrier((weights_own, output_sum))
    pairs = [(0, 1), (1, 0), (2, 3), (3, 2)]
    weights_pair = lax.ppermute(weights_own, "rep", pairs)
    output_grad = lax.psum_scatter(output_sum, "dp", scatter_dimension=1, tiled=True)

    masked_each = masked[None, :, :] * selector[:, :, None]
    lower = jnp.where(odd == 0, weights_own, weights_pair)
    higher = jnp.where(odd == 0, weights_pair, weights_own)
    weights_all = jnp.concatenate([lower, higher], axis=1)
    back = jnp.einsum("erd,efd->rf", masked_each, weights_all, preferred_element_type=jnp.float32)
    grad_gate = (back * upper * sigmoid_gate * (1.0 + gate * (1.0 - sigmoid_gate))).astype(
        jnp.bfloat16
    )
    grad_up = (back * gate * sigmoid_gate).astype(jnp.bfloat16)
    gate_up = jnp.concatenate([grad_gate, grad_up], axis=1)
    gate_up_each = gate_up[None, :, :] * selector[:, :, None]
    input_part = jnp.einsum(
        "erf,rd->efd", gate_up_each, token_inputs, preferred_element_type=jnp.float32
    ).astype(jnp.bfloat16)
    input_sum = rep_sum(input_part, 128)
    input_grad = lax.psum_scatter(input_sum, "dp", scatter_dimension=1, tiled=True)

    whole = gather_matrix(input_grad, output_grad, n_dp)
    finished = whole_sweeps(whole, ITERS, jnp.sqrt(jnp.float32(D)))
    spread = spread_matrix(finished, n_dp)
    return spread.reshape(experts_here, 3, hidden_width, width // n_dp)


def solution(mesh):
    placed = (
        P(("dp", "rep"), None),
        P(("dp", "rep"), None),
        P(("dp", "rep"), None),
        P(("dp", "rep"), None),
        P(None, None, "dp"),
        P(("dp", "rep")),
        P(("dp", "rep")),
    )
    return jax.shard_map(
        per_device, mesh=mesh, in_specs=placed, out_specs=P(None, None, None, "dp"), check_vma=False
    )
```

```python
import functools

import jax
import jax.numpy as jnp
from jax import lax
from jax.experimental import pallas as pl
from jax.experimental.pallas import tpu as pltpu
from jax.sharding import PartitionSpec as P

D = 2048
ITERS = 2
MESH = pl.DeviceIdType.MESH

ns_first = 3.4445
ns_second = -4.775
ns_third = 2.0315
norm_eps = 1e-07


def rep_sum_kernel(
    n_chunks, parts, out, local, near, summed, far,
    load_sem, near_send, near_recv, far_send, far_recv, store_sem,
):
    dp = lax.axis_index("dp")
    rep = lax.axis_index("rep")
    pair = rep + 1 - 2 * lax.rem(rep, 2)
    other = lax.rem(rep + 2, 4)
    other_pair = lax.rem(pair + 2, 4)

    def near_copy(slot, chunk):
        part = other_pair if slot == 0 else pair
        return pltpu.make_async_remote_copy(
            src_ref=parts.at[part, chunk],
            dst_ref=near.at[slot, chunk],
            send_sem=near_send.at[slot, chunk],
            recv_sem=near_recv.at[slot, chunk],
            device_id=(dp, pair),
            device_id_type=MESH,
        )

    def load(slot, chunk):
        part = other if slot == 0 else rep
        return pltpu.make_async_copy(
            parts.at[part, chunk], local.at[slot, chunk], load_sem.at[slot, chunk]
        )

    def far_copy(chunk):
        return pltpu.make_async_remote_copy(
            src_ref=summed.at[chunk],
            dst_ref=far.at[chunk],
            send_sem=far_send.at[chunk],
            recv_sem=far_recv.at[chunk],
            device_id=(dp, other),
            device_id_type=MESH,
        )

    def store(chunk):
        return pltpu.make_async_copy(local.at[1, chunk], out.at[chunk], store_sem.at[chunk])

    for slot in range(2):

        @pl.loop(0, n_chunks)
        def _(chunk, slot=slot):
            near_copy(slot, chunk).start()
            load(slot, chunk).start()

    @pl.loop(0, n_chunks)
    def _(chunk):
        load(0, chunk).wait()
        near_copy(0, chunk).wait_recv()
        summed[chunk] = (
            local[0, chunk].astype(jnp.float32) + near[0, chunk].astype(jnp.float32)
        ).astype(jnp.bfloat16)
        far_copy(chunk).start()

    @pl.loop(0, n_chunks)
    def _(chunk):
        load(1, chunk).wait()
        near_copy(1, chunk).wait_recv()
        far_copy(chunk).wait_recv()
        local[1, chunk] = (
            local[1, chunk].astype(jnp.float32)
            + near[1, chunk].astype(jnp.float32)
            + far[chunk].astype(jnp.float32)
        ).astype(jnp.bfloat16)
        store(chunk).start()

    @pl.loop(0, n_chunks)
    def _(chunk):
        near_copy(0, chunk).wait_send()
        near_copy(1, chunk).wait_send()
        far_copy(chunk).wait_send()
        store(chunk).wait()


def rep_sum(value, rows):
    width = value.shape[-1]
    parts = value.reshape(4, -1, rows, width)
    n_chunks = parts.shape[1]
    block = (n_chunks, rows, width)
    summed = pl.pallas_call(
        functools.partial(rep_sum_kernel, n_chunks),
        out_shape=jax.ShapeDtypeStruct(block, jnp.bfloat16),
        in_specs=[pl.BlockSpec(memory_space=pl.ANY)],
        out_specs=pl.BlockSpec(memory_space=pl.ANY),
        scratch_shapes=[
            pltpu.VMEM((2,) + block, jnp.bfloat16),
            pltpu.VMEM((2,) + block, jnp.bfloat16),
            pltpu.VMEM(block, jnp.bfloat16),
            pltpu.VMEM(block, jnp.bfloat16),
            pltpu.SemaphoreType.DMA((2, n_chunks)),
            pltpu.SemaphoreType.DMA((2, n_chunks)),
            pltpu.SemaphoreType.DMA((2, n_chunks)),
            pltpu.SemaphoreType.DMA((n_chunks,)),
            pltpu.SemaphoreType.DMA((n_chunks,)),
            pltpu.SemaphoreType.DMA((n_chunks,)),
        ],
        compiler_params=pltpu.CompilerParams(has_side_effects=True),
        cost_estimate=pl.CostEstimate(
            flops=value.size * 1000, bytes_accessed=value.size * 2, transcendentals=0
        ),
    )(parts)
    return summed.reshape(n_chunks * rows, width)


def full_sum_kernel(
    n_chunks, n_dp, parts, out, local, near, summed, far, blocks,
    load_sem, near_send, near_recv, far_send, far_recv, block_send, block_recv,
):
    dp = lax.axis_index("dp")
    rep = lax.axis_index("rep")
    pair = rep + 1 - 2 * lax.rem(rep, 2)
    other = lax.rem(rep + 2, 4)
    other_pair = lax.rem(pair + 2, 4)
    width = blocks.shape[-1]

    def near_copy(slot, chunk):
        part = other_pair if slot == 0 else pair
        return pltpu.make_async_remote_copy(
            src_ref=parts.at[part, chunk],
            dst_ref=near.at[slot, chunk],
            send_sem=near_send.at[slot, chunk],
            recv_sem=near_recv.at[slot, chunk],
            device_id=(dp, pair),
            device_id_type=MESH,
        )

    def load(slot, chunk):
        part = other if slot == 0 else rep
        return pltpu.make_async_copy(
            parts.at[part, chunk], local.at[slot, chunk], load_sem.at[slot, chunk]
        )

    def far_copy(chunk):
        return pltpu.make_async_remote_copy(
            src_ref=summed.at[chunk],
            dst_ref=far.at[chunk],
            send_sem=far_send.at[chunk],
            recv_sem=far_recv.at[chunk],
            device_id=(dp, other),
            device_id_type=MESH,
        )

    def columns(block):
        return pl.ds(pl.multiple_of(block * width, width), width)

    def block_copy(chunk, target, source):
        return pltpu.make_async_remote_copy(
            src_ref=local.at[1, chunk, :, columns(target)],
            dst_ref=blocks.at[chunk, source],
            send_sem=block_send.at[chunk, target],
            recv_sem=block_recv.at[chunk, source],
            device_id=(target, rep),
            device_id_type=MESH,
        )

    def own_copy(chunk):
        return pltpu.make_async_copy(
            local.at[1, chunk, :, columns(dp)], blocks.at[chunk, dp], block_recv.at[chunk, dp]
        )

    for slot in range(2):

        @pl.loop(0, n_chunks)
        def _(chunk, slot=slot):
            near_copy(slot, chunk).start()
            load(slot, chunk).start()

    @pl.loop(0, n_chunks)
    def _(chunk):
        load(0, chunk).wait()
        near_copy(0, chunk).wait_recv()
        summed[chunk] = (
            local[0, chunk].astype(jnp.float32) + near[0, chunk].astype(jnp.float32)
        ).astype(jnp.bfloat16)
        far_copy(chunk).start()

    @pl.loop(0, n_chunks)
    def _(chunk):
        load(1, chunk).wait()
        near_copy(1, chunk).wait_recv()
        far_copy(chunk).wait_recv()
        local[1, chunk] = (
            local[1, chunk].astype(jnp.float32)
            + near[1, chunk].astype(jnp.float32)
            + far[chunk].astype(jnp.float32)
        ).astype(jnp.bfloat16)
        for step in range(1, n_dp):
            block_copy(chunk, lax.rem(dp + step, n_dp), dp).start()
        own_copy(chunk).start()

    @pl.loop(0, n_chunks)
    def _(chunk):
        own_copy(chunk).wait()
        for step in range(1, n_dp):
            block_copy(chunk, dp, lax.rem(dp + step, n_dp)).wait_recv()
        total = blocks[chunk, 0].astype(jnp.float32)
        for source in range(1, n_dp):
            total = total + blocks[chunk, source].astype(jnp.float32)
        out[chunk] = total.astype(jnp.bfloat16)

    @pl.loop(0, n_chunks)
    def _(chunk):
        near_copy(0, chunk).wait_send()
        near_copy(1, chunk).wait_send()
        far_copy(chunk).wait_send()
        for step in range(1, n_dp):
            block_copy(chunk, lax.rem(dp + step, n_dp), dp).wait_send()


def full_sum(value, rows, n_dp):
    width = value.shape[-1]
    own = width // n_dp
    if own % 128 != 0:
        return lax.psum_scatter(rep_sum(value, rows), "dp", scatter_dimension=1, tiled=True)
    parts = value.reshape(4, -1, rows, width)
    n_chunks = parts.shape[1]
    block = (n_chunks, rows, width)
    summed = pl.pallas_call(
        functools.partial(full_sum_kernel, n_chunks, n_dp),
        out_shape=jax.ShapeDtypeStruct((n_chunks, rows, own), jnp.bfloat16),
        in_specs=[pl.BlockSpec(memory_space=pl.ANY)],
        out_specs=pl.BlockSpec(memory_space=pltpu.VMEM),
        scratch_shapes=[
            pltpu.VMEM((2,) + block, jnp.bfloat16),
            pltpu.VMEM((2,) + block, jnp.bfloat16),
            pltpu.VMEM(block, jnp.bfloat16),
            pltpu.VMEM(block, jnp.bfloat16),
            pltpu.VMEM((n_chunks, n_dp, rows, own), jnp.bfloat16),
            pltpu.SemaphoreType.DMA((2, n_chunks)),
            pltpu.SemaphoreType.DMA((2, n_chunks)),
            pltpu.SemaphoreType.DMA((2, n_chunks)),
            pltpu.SemaphoreType.DMA((n_chunks,)),
            pltpu.SemaphoreType.DMA((n_chunks,)),
            pltpu.SemaphoreType.DMA((n_chunks, n_dp)),
            pltpu.SemaphoreType.DMA((n_chunks, n_dp)),
        ],
        compiler_params=pltpu.CompilerParams(has_side_effects=True),
        cost_estimate=pl.CostEstimate(
            flops=value.size * 1000, bytes_accessed=value.size * 2, transcendentals=0
        ),
    )(parts)
    return summed.reshape(n_chunks * rows, own)


def column_block(matrix, source, width, rows=None):
    if len(matrix.shape) == 3:
        return matrix.at[source] if rows is None else matrix.at[source, rows]
    start = source * width
    cols = pl.ds(start if isinstance(start, int) else pl.multiple_of(start, width), width)
    return matrix.at[:, cols] if rows is None else matrix.at[rows, cols]


def gather_kernel(n_dp, first, second, whole, full_send, half_send, full_recv, half_recv):
    dp = lax.axis_index("dp")
    rep = lax.axis_index("rep")
    odd = lax.rem(rep, 2)
    hidden, width = first.shape
    half = second.shape[0]
    owner = n_dp // 4

    def full_copy(source):
        return pltpu.make_async_remote_copy(
            src_ref=first,
            dst_ref=column_block(whole, source, width),
            send_sem=full_send,
            recv_sem=full_recv.at[source],
            device_id=(owner + odd, rep),
            device_id_type=MESH,
        )

    def half_copy(place, source):
        rows = pl.ds(pl.multiple_of(place * half, half), half)
        return pltpu.make_async_remote_copy(
            src_ref=second,
            dst_ref=column_block(whole, source, width, rows),
            send_sem=half_send,
            recv_sem=half_recv.at[place, source],
            device_id=(owner + 2, rep - odd),
            device_id_type=MESH,
        )

    own_full = pltpu.make_async_copy(first, column_block(whole, dp, width), full_send)
    own_half = pltpu.make_async_copy(
        second, column_block(whole, dp, width, pl.ds(0, half)), half_send
    )
    is_full = dp == owner + odd
    is_half = jnp.logical_and(dp == owner + 2, odd == 0)

    @pl.when(is_full)
    def _():
        own_full.start()

    @pl.when(jnp.logical_not(is_full))
    def _():
        full_copy(dp).start()

    @pl.when(is_half)
    def _():
        own_half.start()

    @pl.when(jnp.logical_not(is_half))
    def _():
        half_copy(odd, dp).start()

    @pl.when(is_full)
    def _():
        own_full.wait()
        for source in range(n_dp):

            @pl.when(dp != source)
            def _(source=source):
                full_copy(source).wait_recv()

    @pl.when(jnp.logical_not(is_full))
    def _():
        full_copy(dp).wait_send()

    @pl.when(is_half)
    def _():
        own_half.wait()
        for source in range(n_dp):
            half_copy(1, source).wait_recv()

            @pl.when(dp != source)
            def _(source=source):
                half_copy(0, source).wait_recv()

    @pl.when(jnp.logical_not(is_half))
    def _():
        half_copy(odd, dp).wait_send()


def gather_matrix(first, second, n_dp):
    hidden, width = first.shape
    blocked = width % 128 != 0
    shape = (n_dp, hidden, width) if blocked else (hidden, width * n_dp)
    whole = pl.pallas_call(
        functools.partial(gather_kernel, n_dp),
        out_shape=jax.ShapeDtypeStruct(shape, jnp.bfloat16),
        in_specs=[pl.BlockSpec(memory_space=pltpu.VMEM)] * 2,
        out_specs=pl.BlockSpec(memory_space=pltpu.VMEM),
        scratch_shapes=[
            pltpu.SemaphoreType.DMA,
            pltpu.SemaphoreType.DMA,
            pltpu.SemaphoreType.DMA((n_dp,)),
            pltpu.SemaphoreType.DMA((2, n_dp)),
        ],
        compiler_params=pltpu.CompilerParams(has_side_effects=True),
    )(first, second)
    return whole.transpose(1, 0, 2).reshape(hidden, width * n_dp) if blocked else whole


def spread_kernel(n_dp, matrix, out, held, owner_send, pair_send, far_send, recv, store_sem):
    dp = lax.axis_index("dp")
    rep = lax.axis_index("rep")
    half, width = held.shape[1:]
    owner = n_dp // 4
    pair = rep + 1 - 2 * lax.rem(rep, 2)
    other = lax.rem(rep + 2, 4)
    kinds = 3
    matrices = {
        2 * (kinds * expert + kind) + place: (expert, kind)
        for place in range(2)
        for expert in range(2)
        for kind in range(kinds)
    }

    def remote(source, index, send_sem, device):
        return pltpu.make_async_remote_copy(
            src_ref=source,
            dst_ref=held.at[index],
            send_sem=send_sem,
            recv_sem=recv.at[index],
            device_id=device,
            device_id_type=MESH,
        )

    def store(index):
        return pltpu.make_async_copy(held.at[index], out.at[index], store_sem.at[index])

    def rows_of(index):
        return pl.ds(index % 2 * half, half)

    def root_of(expert, kind):
        return 2 * expert + kind % 2

    for index, (expert, kind) in matrices.items():

        @pl.when(jnp.logical_and(dp == owner + kind, rep == root_of(expert, kind)))
        def _(index=index, kind=kind):
            for target in sorted(range(n_dp), key=lambda place: -abs(place - owner - kind)):
                block = column_block(matrix, target, width, rows_of(index))

                @pl.when(dp != target)
                def _(target=target, block=block):
                    remote(block, index, owner_send.at[index % 2, target], (target, rep)).start()

                @pl.when(dp == target)
                def _(target=target, block=block):
                    pltpu.make_async_copy(
                        block, held.at[index], owner_send.at[index % 2, target]
                    ).start()

    def arrived(index, expert, kind):
        here = dp == owner + kind

        @pl.when(here)
        def _():
            pltpu.make_async_copy(
                column_block(matrix, dp, width, rows_of(index)),
                held.at[index],
                owner_send.at[index % 2, dp],
            ).wait()

        @pl.when(jnp.logical_not(here))
        def _():
            remote(held.at[index], index, pair_send.at[index], (dp, pair)).wait_recv()

    for index, (expert, kind) in matrices.items():

        @pl.when(rep == root_of(expert, kind))
        def _(index=index, expert=expert, kind=kind):
            arrived(index, expert, kind)
            remote(held.at[index], index, far_send.at[index], (dp, other)).start()
            remote(held.at[index], index, pair_send.at[index], (dp, pair)).start()
            store(index).start()

    for index, (expert, kind) in matrices.items():

        @pl.when(other == root_of(expert, kind))
        def _(index=index):
            remote(held.at[index], index, pair_send.at[index], (dp, pair)).wait_recv()
            remote(held.at[index], index, pair_send.at[index], (dp, pair)).start()
            store(index).start()

    for index, (expert, kind) in matrices.items():
        root = root_of(expert, kind)

        @pl.when(jnp.logical_and(rep != root, other != root))
        def _(index=index):
            remote(held.at[index], index, pair_send.at[index], (dp, pair)).wait_recv()
            store(index).start()

    for index, (expert, kind) in matrices.items():
        root = root_of(expert, kind)

        @pl.when(jnp.logical_and(dp == owner + kind, rep == root))
        def _(index=index):
            for target in range(n_dp):

                @pl.when(dp != target)
                def _(target=target):
                    remote(
                        column_block(matrix, target, width, rows_of(index)),
                        index,
                        owner_send.at[index % 2, target],
                        (target, rep),
                    ).wait_send()

        @pl.when(rep == root)
        def _(index=index):
            remote(held.at[index], index, far_send.at[index], (dp, other)).wait_send()

        @pl.when(jnp.logical_or(rep == root, other == root))
        def _(index=index):
            remote(held.at[index], index, pair_send.at[index], (dp, pair)).wait_send()

        store(index).wait()


def spread_matrix(matrix, n_dp):
    hidden, width = matrix.shape[0], matrix.shape[1] // n_dp
    half = hidden // 2
    if width % 128 != 0:
        matrix = matrix.reshape(hidden, n_dp, width).transpose(1, 0, 2)
    return pl.pallas_call(
        functools.partial(spread_kernel, n_dp),
        out_shape=jax.ShapeDtypeStruct((12, half, width), jnp.bfloat16),
        in_specs=[pl.BlockSpec(memory_space=pltpu.VMEM)],
        out_specs=pl.BlockSpec(memory_space=pl.ANY),
        scratch_shapes=[
            pltpu.VMEM((12, half, width), jnp.bfloat16),
            pltpu.SemaphoreType.DMA((2, n_dp)),
            pltpu.SemaphoreType.DMA((12,)),
            pltpu.SemaphoreType.DMA((12,)),
            pltpu.SemaphoreType.DMA((12,)),
            pltpu.SemaphoreType.DMA((12,)),
        ],
        compiler_params=pltpu.CompilerParams(has_side_effects=True),
    )(matrix)


def whole_sweeps(grad, sweeps, scale):
    as_float = grad.astype(jnp.float32)
    norm = jnp.sqrt(jnp.sum(as_float * as_float)) + norm_eps
    current = (as_float / norm).astype(jnp.bfloat16)
    result = None
    for sweep in range(sweeps):
        gram = jnp.einsum("fd,gd->fg", current, current, preferred_element_type=jnp.float32)
        gram_half = gram.astype(jnp.bfloat16)
        squared = jnp.dot(gram_half, gram_half, preferred_element_type=jnp.float32)
        poly = (ns_second * gram + ns_third * squared).astype(jnp.bfloat16)
        newer = ns_first * current.astype(jnp.float32) + jnp.dot(
            poly, current, preferred_element_type=jnp.float32
        )
        if sweep + 1 < sweeps:
            current = newer.astype(jnp.bfloat16)
        else:
            result = (scale * newer).astype(jnp.bfloat16)
    return result


def per_device(
    token_inputs, cotangent, gate_preact, up_preact, down_weight, block_expert, block_count
):
    n_dp = lax.axis_size("dp")
    rep = lax.axis_index("rep")
    odd = lax.rem(rep, 2)
    blocks = block_count.shape[0]
    rows_here = token_inputs.shape[0]
    hidden_width = gate_preact.shape[1]
    half = hidden_width // 2
    width = token_inputs.shape[1]
    block_rows = rows_here // blocks
    experts_here = down_weight.shape[0]

    own_half = lax.dynamic_slice_in_dim(down_weight, odd * half, half, 1)
    weights_own = lax.all_gather(own_half, "dp", axis=2, tiled=True)

    row_place = jnp.arange(rows_here, dtype=jnp.int32) % block_rows
    row_count = jnp.broadcast_to(block_count[:, None], (blocks, block_rows)).reshape(rows_here)
    row_expert = jnp.broadcast_to(block_expert[:, None], (blocks, block_rows)).reshape(rows_here)
    live_rows = row_place < row_count
    masked = jnp.where(live_rows[:, None], cotangent, jnp.zeros_like(cotangent))
    gate = gate_preact.astype(jnp.float32)
    upper = up_preact.astype(jnp.float32)
    sigmoid_gate = jax.nn.sigmoid(gate)
    hidden = (gate * sigmoid_gate * upper).astype(jnp.bfloat16)
    selector = (row_expert[None, :] == jnp.arange(experts_here, dtype=jnp.int32)[:, None]).astype(
        jnp.bfloat16
    )
    hidden_each = hidden[None, :, :] * selector[:, :, None]
    output_part = jnp.einsum(
        "erf,rd->efd", hidden_each, masked, preferred_element_type=jnp.float32
    ).astype(jnp.bfloat16)
    output_sum = rep_sum(output_part, 128)
    weights_own, output_sum = lax.optimization_barrier((weights_own, output_sum))
    pairs = [(0, 1), (1, 0), (2, 3), (3, 2)]
    weights_pair = lax.ppermute(weights_own, "rep", pairs)
    output_grad = lax.psum_scatter(output_sum, "dp", scatter_dimension=1, tiled=True)

    masked_each = masked[None, :, :] * selector[:, :, None]
    lower = jnp.where(odd == 0, weights_own, weights_pair)
    higher = jnp.where(odd == 0, weights_pair, weights_own)
    weights_all = jnp.concatenate([lower, higher], axis=1)
    back = jnp.einsum("erd,efd->rf", masked_each, weights_all, preferred_element_type=jnp.float32)
    grad_gate = (back * upper * sigmoid_gate * (1.0 + gate * (1.0 - sigmoid_gate))).astype(
        jnp.bfloat16
    )
    grad_up = (back * gate * sigmoid_gate).astype(jnp.bfloat16)
    gate_up = jnp.concatenate([grad_gate, grad_up], axis=1)
    gate_up_each = gate_up[None, :, :] * selector[:, :, None]
    input_part = jnp.einsum(
        "erf,rd->efd", gate_up_each, token_inputs, preferred_element_type=jnp.float32
    ).astype(jnp.bfloat16)
    input_grad = full_sum(input_part, 96, n_dp)

    whole = gather_matrix(input_grad, output_grad, n_dp)
    finished = whole_sweeps(whole, ITERS, jnp.sqrt(jnp.float32(D)))
    spread = spread_matrix(finished, n_dp)
    return spread.reshape(experts_here, 3, hidden_width, width // n_dp)


def solution(mesh):
    placed = (
        P(("dp", "rep"), None),
        P(("dp", "rep"), None),
        P(("dp", "rep"), None),
        P(("dp", "rep"), None),
        P(None, None, "dp"),
        P(("dp", "rep")),
        P(("dp", "rep")),
    )
    return jax.shard_map(
        per_device, mesh=mesh, in_specs=placed, out_specs=P(None, None, None, "dp"), check_vma=False
    )
```
